32 devices in a mesh: gx: 4 (over x, core), gy: 4 (over z), gz: 2 (over y).
Axes of the slice: x: 2, y: 2, z: 4, core: 2. Of those that a mesh axis runs over, the one named last changes fastest.
Arguments:
- divergence: float32 [64, 64, 256], P('gx', 'gy', 'gz'), may hold values from -6 to 6
- damping: float32 [64, 64, 256], P('gx', 'gy', 'gz'), may hold values from 5e-06 to 0.004
Outputs:
- potential: float32 [64, 64, 256], P('gx', 'gy', 'gz')
The draws below stay inside these ranges and needn't reach their ends.
All inputs are finite; a program needn't handle non-finite values.
Results may differ from the reference program's by a relative error of at most 0.0001.
Values sent between devices are 32-bit elements; how exact they have to be, the bound alone decides.
A program may use at most 64 MiB of HBM per device.

```python
import math
import jax
import jax.numpy as jnp
from jax import lax

CX = 16
CY = 16
CZ = 128
LEVELS = 4
PRE = 2
POST = 2
NX = 64
NY = 64
NZ = 256


def smooth_field(key, size_x, size_y, size_z):
    keys = jax.random.split(key, 3)
    freqs = jax.random.randint(keys[0], (3, 3), 1, 3).astype(jnp.float32)
    phases = jax.random.uniform(keys[1], (3, 3), jnp.float32, 0.0, 2.0 * math.pi)
    weights = jax.random.uniform(keys[2], (3,), jnp.float32, 0.5, 1.0)
    coord_x = (jnp.arange(size_x, dtype=jnp.float32) + 0.5) / size_x
    coord_y = (jnp.arange(size_y, dtype=jnp.float32) + 0.5) / size_y
    coord_z = (jnp.arange(size_z, dtype=jnp.float32) + 0.5) / size_z
    total = jnp.zeros((size_x, size_y, size_z), jnp.float32)
    for term_index in range(3):
        along_x = jnp.cos(2.0 * math.pi * freqs[term_index, 0] * coord_x + phases[term_index, 0])
        along_y = jnp.cos(2.0 * math.pi * freqs[term_index, 1] * coord_y + phases[term_index, 1])
        along_z = jnp.cos(2.0 * math.pi * freqs[term_index, 2] * coord_z + phases[term_index, 2])
        total = total + weights[term_index] * along_x[:, None, None] * along_y[None, :, None] * along_z[None, None, :]
    return total / jnp.sum(weights)


def draw_divergence(key, part):
    rough_key = jax.random.fold_in(key, 11)
    smooth_key = jax.random.fold_in(key, 12)
    strength = 2.0 * (9.87 * (1.0 / (NX * NX) + 1.0 / (NY * NY) + 1.0 / (NZ * NZ)) + 0.0003)
    smooth = smooth_field(smooth_key, NX, NY, NZ)
    rough = jnp.clip(jax.random.normal(rough_key, (NX, NY, NZ), jnp.float32), -4.0, 4.0)
    broad = strength * 2.0 * smooth
    return rough + broad


def draw_damping(key, part):
    rough_key = jax.random.fold_in(key, 21)
    smooth_key = jax.random.fold_in(key, 22)
    smooth = smooth_field(smooth_key, NX, NY, NZ)
    rough = jnp.tanh(jax.random.normal(rough_key, (NX, NY, NZ), jnp.float32))
    share = 0.5 + 0.299 * rough + 0.2 * smooth
    return jnp.exp(math.log(5e-06) + math.log(800.0) * share)


def setup_inputs(seed: int = 0) -> dict:
    splits = jax.random.split(jax.random.key(seed), 3)
    return {
        "divergence": draw_divergence(jax.random.fold_in(splits[2], 71), 0),
        "damping": draw_damping(jax.random.fold_in(splits[2], 71), 0),
    }


relax_weight = 2.0 / 3.0

def neighbour_sum(padded):
    total = padded[2:, 1:-1, 1:-1] + padded[:-2, 1:-1, 1:-1]
    total = total + padded[1:-1, 2:, 1:-1] + padded[1:-1, :-2, 1:-1]
    total = total + padded[1:-1, 1:-1, 2:] + padded[1:-1, 1:-1, :-2]
    return total

def apply_level(values, padded, damping_level, coupling):
    return (6.0 * values - neighbour_sum(padded)) * coupling + damping_level * values

def relaxed_sweep(values, padded, source, damping_level, coupling):
    diagonal = 6.0 * coupling + damping_level
    return values + relax_weight * (source - apply_level(values, padded, damping_level, coupling)) / diagonal

def coarsen(values, block_x, block_y, block_z):
    size_x, size_y, size_z = values.shape
    shaped = values.reshape(size_x // block_x, block_x, size_y // block_y, block_y, size_z // block_z, block_z)
    return shaped.mean(axis=(1, 3, 5))

def refine(values, block_x, block_y, block_z):
    return jnp.repeat(jnp.repeat(jnp.repeat(values, block_x, 0), block_y, 1), block_z, 2)

def sine_table(points, dtype):
    indices = jnp.arange(points, dtype=dtype) + 1.0
    return math.sqrt(2.0 / (points + 1)) * jnp.sin(math.pi * indices[:, None] * indices[None, :] / (points + 1))

def eigen_values(points, spacing, dtype):
    indices = jnp.arange(points, dtype=dtype) + 1.0
    return (2.0 - 2.0 * jnp.cos(math.pi * indices / (points + 1))) / (spacing * spacing)

def coarse_solve(source, damping_mean, spacing_x, spacing_y, spacing_z):
    size_x, size_y, size_z = source.shape
    dtype = source.dtype
    table_x = sine_table(size_x, dtype)
    table_y = sine_table(size_y, dtype)
    table_z = sine_table(size_z, dtype)
    spectrum = jnp.einsum('ai,bj,ck,ijk->abc', table_x, table_y, table_z, source, precision=lax.Precision.HIGHEST)
    denominator = eigen_values(size_x, spacing_x, dtype)[:, None, None] + eigen_values(size_y, spacing_y, dtype)[None, :, None] + eigen_values(size_z, spacing_z, dtype)[None, None, :] + damping_mean
    spectrum = spectrum / denominator
    return jnp.einsum('ia,jb,kc,abc->ijk', table_x, table_y, table_z, spectrum, precision=lax.Precision.HIGHEST)

def reference(divergence, damping):
    dampings = [damping]
    for level_index in range(1, LEVELS):
        dampings.append(coarsen(dampings[-1], 2, 2, 2))
    sources = []
    smoothed = []
    source = divergence
    for level_index in range(LEVELS):
        coupling = 0.25 ** level_index
        values = relax_weight * source / (6.0 * coupling + dampings[level_index])
        for sweep_index in range(PRE - 1):
            values = relaxed_sweep(values, jnp.pad(values, 1), source, dampings[level_index], coupling)
        remainder = source - apply_level(values, jnp.pad(values, 1), dampings[level_index], coupling)
        sources.append(source)
        smoothed.append(values)
        source = coarsen(remainder, 2, 2, 2)
    shrink = 2 ** (LEVELS - 1)
    block_x, block_y, block_z = (CX // shrink, CY // shrink, CZ // shrink)
    coarse_source = coarsen(remainder, block_x, block_y, block_z)
    damping_mean = jnp.mean(coarsen(dampings[-1], block_x, block_y, block_z))
    solution = coarse_solve(coarse_source, damping_mean, CX, CY, CZ)
    correction = refine(solution, block_x, block_y, block_z)
    for level_index in reversed(range(LEVELS)):
        coupling = 0.25 ** level_index
        values = smoothed[level_index] + correction
        for sweep_index in range(POST):
            values = relaxed_sweep(values, jnp.pad(values, 1), sources[level_index], dampings[level_index], coupling)
        if level_index > 0:
            correction = refine(values, 2, 2, 2)
    return values
```

```python
import functools
import math

import jax
import jax.numpy as jnp
import numpy as np
from jax import lax
from jax.experimental import pallas as pl
from jax.experimental.pallas import tpu as pltpu
from jax.sharding import PartitionSpec as P

AXES = ("gx", "gy", "gz")
ROUNDS = 7
WEIGHT = 2.0 / 3.0
MESH = pl.DeviceIdType.MESH
HIGH = lax.Precision.HIGHEST


def dot(a, b, dims=(((1,), (0,)), ((), ()))):
    return lax.dot_general(a, b, dims, precision=HIGH, preferred_element_type=jnp.float32)


def one_hot(condition):
    return jnp.where(condition, 1.0, 0.0).astype(jnp.float32)


def iota(shape, dim):
    return lax.broadcasted_iota(jnp.int32, shape, dim)


def coarsen_dup(values, step):
    nx, ny, nz = values.shape
    pairs = values.reshape(nx // 2, 2, ny, nz)
    total = pairs[:, 0] + pairs[:, 1]
    for dim, size in ((1, ny), (2, nz)):
        even = (iota(total.shape, dim) // step) % 2 == 0
        total = total + jnp.where(
            even, pltpu.roll(total, size - step, dim), pltpu.roll(total, step, dim)
        )
    return total * 0.125


def expand_x(values, times):
    nx, ny, nz = values.shape
    return jnp.broadcast_to(values[:, None], (nx, times, ny, nz)).reshape(nx * times, ny, nz)


def sum_x(values, low, high):
    return jnp.concatenate([low[None], values[:-1]], 0) + jnp.concatenate(
        [values[1:], high[None]], 0
    )


def neighbours_global(values, step, valid_z):
    nx, ny, nz = values.shape
    zero = jnp.zeros((ny, nz), jnp.float32)
    total = sum_x(values, zero, zero)
    row, lane = iota(values.shape, 1), iota(values.shape, 2)
    total = total + jnp.where(row < step, 0.0, pltpu.roll(values, step, 1))
    total = total + jnp.where(row >= ny - step, 0.0, pltpu.roll(values, ny - step, 1))
    total = total + jnp.where(lane < step, 0.0, pltpu.roll(values, step, 2))
    total = total + jnp.where(lane >= valid_z - step, 0.0, pltpu.roll(values, nz - step, 2))
    return total


def kernel(
    counts, tables, b_ref, d_ref, ty_ref, tz_ref, den_ref, out_ref,
    xsend, ysend, zsend, xrecv, yrecv, zrecv, pay, gathered, gb, gd, v2,
    ssem, rsem, gssem, grsem,
):
    cx, cy, cz = counts
    table_x = tables
    nx, ny, nz = (lax.axis_size(a) for a in AXES)
    devices = nx * ny * nz
    gx, gy, gz = (lax.axis_index(a) for a in AXES)
    place = {"gx": gx, "gy": gy, "gz": gz}
    size = {"gx": nx, "gy": ny, "gz": nz}
    me = (gx * ny + gy) * nz + gz

    def coords(index):
        return (index // (ny * nz), (index // nz) % ny, index % nz)

    xrecv[...] = jnp.zeros_like(xrecv)
    yrecv[...] = jnp.zeros_like(yrecv)
    zrecv[...] = jnp.zeros_like(zrecv)

    barrier = pltpu.get_barrier_semaphore()

    @pl.loop(1, devices)
    def _(k):
        pl.semaphore_signal(
            barrier, inc=1, device_id=coords((me + k) % devices), device_id_type=MESH
        )

    b0 = b_ref[...]
    d0 = d_ref[...]

    pl.semaphore_wait(barrier, devices - 1)

    def copies(r, level_x):
        result = []
        for axis_number, (axis, send, recv, length) in enumerate(
            (("gx", xsend, xrecv, cy), ("gy", ysend, yrecv, level_x), ("gz", zsend, zrecv, None))
        ):
            for side in (0, 1):
                other = 1 - side
                index = 2 * axis_number
                if length is None:
                    src = send.at[r]
                    there, here = recv.at[r, other], recv.at[r, side]
                    if level_x * cy < send.shape[2]:
                        cut = (slice(None), pl.ds(0, level_x * cy))
                        src, there, here = src.at[cut], there.at[cut], here.at[cut]
                else:
                    cut = pl.ds(0, length)
                    src = send.at[r, side, cut]
                    there, here = recv.at[r, other, cut], recv.at[r, side, cut]
                target = dict(place)
                target[axis] = place[axis] + (1 if side else -1)
                device = tuple(target[a] for a in AXES)
                exists = place[axis] < size[axis] - 1 if side else place[axis] > 0
                out = pltpu.make_async_remote_copy(
                    src, there, ssem.at[r, index + side], rsem.at[r, index + other], device, MESH
                )
                back = pltpu.make_async_remote_copy(
                    src, here, ssem.at[r, index + side], rsem.at[r, index + side], device, MESH
                )
                result.append((exists, out, back))
        return result

    def exchange(r, values):
        level_x = values.shape[0]
        rows = level_x * cy
        xsend[r, 0] = values[0]
        xsend[r, 1] = values[-1]
        ysend[r, 0, 0:level_x] = values[:, 0, :]
        ysend[r, 1, 0:level_x] = values[:, cy - 1, :]
        pick = one_hot(iota((8, cz), 1) == jnp.where(iota((8, cz), 0) == 0, 0, cz - 1))
        pick = jnp.where(iota((8, cz), 0) < 2, pick, 0.0)
        zsend[r, :, 0:rows] = dot(pick, values.reshape(rows, cz), (((1,), (1,)), ((), ())))
        for exists, out, _ in copies(r, level_x):
            pl.when(exists)(out.start)

    def neighbours(r, values, step):
        level_x = values.shape[0]
        rows = level_x * cy
        row, lane = iota(values.shape, 1), iota(values.shape, 2)
        total = jnp.where(lane < step, 0.0, pltpu.roll(values, step, 2))
        total = total + jnp.where(lane >= cz - step, 0.0, pltpu.roll(values, cz - step, 2))
        up, down = pltpu.roll(values, step, 1), pltpu.roll(values, cy - step, 1)
        for exists, _, back in copies(r, level_x):
            pl.when(exists)(back.wait_recv)
        total = total + sum_x(values, xrecv[r, 0], xrecv[r, 1])
        low, high = yrecv[r, 0, 0:level_x], yrecv[r, 1, 0:level_x]
        total = total + jnp.where(row < step, low[:, None, :], up)
        total = total + jnp.where(row >= cy - step, high[:, None, :], down)
        halo = jnp.concatenate([zrecv[r, 0, :, 0:rows], zrecv[r, 1, :, 0:rows]], 0)
        slot, at = iota((16, cz), 0), iota((16, cz), 1)
        spread = one_hot(((slot == 1) & (at < step)) | ((slot == 8) & (at >= cz - step)))
        edge = dot(halo.T, spread)
        return total + edge.reshape(level_x, cy, cz)

    def sweep(values, around, source, scaled, coupling):
        return values * (1.0 - WEIGHT) + scaled * (source + coupling * around)

    diag0 = 6.0 + d0
    scaled0 = WEIGHT / diag0
    v = scaled0 * b0
    exchange(0, v)
    d1 = coarsen_dup(d0, 1)
    d2 = coarsen_dup(d1, 2)
    s0 = sweep(v, neighbours(0, v, 1), b0, scaled0, 1.0)
    exchange(1, s0)
    b1 = coarsen_dup(b0 - diag0 * s0 + neighbours(1, s0, 1), 1)

    diag1 = 1.5 + d1
    scaled1 = WEIGHT / diag1
    v = scaled1 * b1
    exchange(2, v)
    s1 = sweep(v, neighbours(2, v, 2), b1, scaled1, 0.25)
    exchange(3, s1)
    around1 = neighbours(3, s1, 2)
    b2 = coarsen_dup(b1 - diag1 * s1 + 0.25 * around1, 2)

    qx, qy, qz = cx // 4, cy // 4, cz // 4
    row, lane = iota((cz, cz), 0), iota((cz, cz), 1)
    for which, block in enumerate((b2, d2)):
        flat = jnp.zeros((cy, cz), jnp.float32)
        for x in range(qx):
            place_z = one_hot((lane // qz == x) & (row == 4 * (lane % qz)))
            flat = flat + dot(block[x], place_z)
        pick_y = one_hot(iota((8, cy), 1) == 4 * (iota((8, cy), 0) - which * qy))
        if which:
            pay[...] = packed + dot(pick_y * one_hot(iota((8, cy), 0) >= qy), flat)
        else:
            packed = dot(pick_y * one_hot(iota((8, cy), 0) < qy), flat)
    gathered[me] = pay[...]

    def gather_copy(k):
        return pltpu.make_async_remote_copy(
            pay, gathered.at[me], gssem.at[k], grsem.at[me], coords((me + k) % devices), MESH
        )

    @pl.loop(1, devices)
    def _(k):
        gather_copy(k).start()

    @pl.loop(1, devices)
    def _(k):
        origin = (me + devices - k) % devices
        pltpu.make_async_remote_copy(
            pay, gathered.at[origin], gssem.at[k], grsem.at[origin],
            coords((me + k) % devices), MESH,
        ).wait_recv()

    wide = gb.shape[2]
    valid = nz * qz
    per_tile = cz // qz
    blocks = gathered[...].reshape(nx, ny, nz, 8, cz)
    lane = iota((nx, ny, 8, cz), 3)
    for tile in range(wide // cz):
        for x in range(qx):
            total = jnp.zeros((nx, ny, 8, cz), jnp.float32)
            for spot in range(min(per_tile, nz - tile * per_tile)):
                shift = (qz * (spot - x)) % cz
                piece = blocks[:, :, tile * per_tile + spot]
                if shift:
                    piece = pltpu.roll(piece.reshape(nx * ny * 8, cz), shift, 1).reshape(
                        nx, ny, 8, cz
                    )
                total = jnp.where(lane // qz == spot, piece, total)
            for i in range(nx):
                for j in range(ny):
                    where = (qx * i + x, slice(qy * j, qy * j + qy), slice(tile * cz, tile * cz + cz))
                    gb[where] = total[i, j, 0:qy]
                    gd[where] = total[i, j, qy : 2 * qy]
    b2 = gb[...]
    d2 = gd[...]
    damping_mean = jnp.sum(jnp.sum(d2, 0, keepdims=True), axis=(1, 2), keepdims=True)[0] * (
        1.0 / (b2.shape[0] * b2.shape[1] * valid)
    )
    c2, c3 = 0.25**2, 0.25**3
    diag2 = 6.0 * c2 + d2
    scaled2 = WEIGHT / diag2
    v = scaled2 * b2
    s2 = sweep(v, neighbours_global(v, 1, valid), b2, scaled2, c2)
    near2 = neighbours_global(s2, 1, valid)
    b3 = coarsen_dup(b2 - diag2 * s2 + c2 * near2, 1)
    diag3 = 6.0 * c3 + coarsen_dup(d2, 1)
    scaled3 = WEIGHT / diag3
    v = scaled3 * b3
    s3 = sweep(v, neighbours_global(v, 2, valid), b3, scaled3, c3)
    near3 = neighbours_global(s3, 2, valid)
    rem = b3 - diag3 * s3 + c3 * near3

    bx = cx // 8
    rows = rem.shape[1]
    ty, tz = ty_ref[...], tz_ref[...]
    rem = rem.reshape(nx, bx, rows, wide)
    means = rem[:, 0]
    for i in range(1, bx):
        means = means + rem[:, i]
    means = dot(means.reshape(nx * rows, wide), tz).reshape(nx, rows, wide)
    means = [dot(ty, means[i]) for i in range(nx)]
    spectrum = []
    for a in range(nx):
        term = means[0] * float(table_x[a, 0] / bx)
        for i in range(1, nx):
            term = term + means[i] * float(table_x[a, i] / bx)
        spectrum.append(dot(ty, term / (den_ref[a] + damping_mean)))
    solved = []
    for i in range(nx):
        term = spectrum[0] * float(table_x[i, 0])
        for a in range(1, nx):
            term = term + spectrum[a] * float(table_x[i, a])
        solved.append(term)
    solved = dot(jnp.stack(solved).reshape(nx * rows, wide), tz).reshape(nx, rows, wide)

    v = s3 + expand_x(solved, bx)
    for _ in range(2):
        v = sweep(v, neighbours_global(v, 2, valid), b3, scaled3, c3)
    v = s2 + expand_x(v, 2)
    for _ in range(2):
        v = sweep(v, neighbours_global(v, 1, valid), b2, scaled2, c2)

    zero = jnp.zeros((1, rows, wide), jnp.float32)
    v2[0:1] = zero
    v2[pl.ds(1, qx * nx)] = v
    v2[pl.ds(1 + qx * nx, 1)] = zero
    part = v2[pl.ds(qx * gx, qx + 2)]
    k, at = iota((wide, cz), 0), iota((wide, cz), 1)
    inside = k < valid
    fine = at // 2 + gz * (cz // 2)
    own_z = one_hot(inside & (k == fine // 2))
    next_z = one_hot(inside & (k == (fine + 1) // 2)) + one_hot(
        inside & (k == (fine + 1) // 2 - 1)
    )
    at, k = iota((cy, rows), 0), iota((cy, rows), 1)
    fine = at // 2 + gy * (cy // 2)
    own_y = one_hot(k == fine // 2)
    next_y = one_hot(k == (fine + 1) // 2) + one_hot(k == (fine + 1) // 2 - 1)
    in_z = dot(part.reshape((qx + 2) * rows, wide), own_z).reshape(qx + 2, rows, cz)
    by_z = dot(part[1 : qx + 1].reshape(qx * rows, wide), next_z).reshape(qx, rows, cz)
    own = [dot(own_y, in_z[i]) for i in range(qx + 2)]
    side = [dot(next_y, in_z[i + 1]) + dot(own_y, by_z[i]) for i in range(qx)]
    correction = expand_x(jnp.stack(own[1:-1]), 2)
    near = expand_x(jnp.stack(side), 2) + sum_x(correction, own[0], own[-1])
    v = sweep(s1 + correction, around1 + near, b1, scaled1, 0.25)
    exchange(4, v)
    v = sweep(v, neighbours(4, v, 2), b1, scaled1, 0.25)

    v = s0 + expand_x(v, 2)
    exchange(5, v)
    v = sweep(v, neighbours(5, v, 1), b0, scaled0, 1.0)
    exchange(6, v)
    out_ref[...] = sweep(v, neighbours(6, v, 1), b0, scaled0, 1.0)

    for r in range(ROUNDS):
        for exists, out, _ in copies(r, cx // 2 if r in (2, 3, 4) else cx):
            pl.when(exists)(out.wait_send)

    @pl.loop(1, devices)
    def _(k):
        gather_copy(k).wait_send()


def sine_table(points):
    index = np.arange(1, points + 1)
    return math.sqrt(2.0 / (points + 1)) * np.sin(
        math.pi * index[:, None] * index[None, :] / (points + 1)
    )


def eigen_values(points, spacing):
    index = np.arange(1, points + 1)
    return (2.0 - 2.0 * np.cos(math.pi * index / (points + 1))) / (spacing * spacing)


def solution(mesh):
    nx, ny, nz = (mesh.shape[a] for a in AXES)

    def local(divergence, damping):
        cx, cy, cz = divergence.shape
        rows, valid = ny * (cy // 4), nz * (cz // 4)
        wide = -(-valid // cz) * cz
        spread_y, spread_z = cy // 4, cz // 4
        table_y = np.repeat(np.repeat(sine_table(ny), spread_y, 0), spread_y, 1) / spread_y
        table_z = np.zeros((wide, wide))
        table_z[:valid, :valid] = (
            np.repeat(np.repeat(sine_table(nz), spread_z, 0), spread_z, 1) / spread_z
        )
        den = np.ones((nx, rows, wide))
        den[:, :, :valid] = (
            eigen_values(nx, cx)[:, None, None]
            + np.repeat(eigen_values(ny, cy), spread_y)[None, :, None]
            + np.repeat(eigen_values(nz, cz), spread_z)[None, None, :]
        )
        tables = [jnp.asarray(t, jnp.float32) for t in (table_y, table_z, den)]
        f32 = jnp.float32
        devices = nx * ny * nz
        return pl.pallas_call(
            functools.partial(kernel, (cx, cy, cz), sine_table(nx)),
            out_shape=jax.ShapeDtypeStruct(divergence.shape, f32),
            in_specs=[pl.BlockSpec(memory_space=pltpu.VMEM)] * 5,
            out_specs=pl.BlockSpec(memory_space=pltpu.VMEM),
            scratch_shapes=[
                pltpu.VMEM((ROUNDS, 2, cy, cz), f32),
                pltpu.VMEM((ROUNDS, 2, cx, cz), f32),
                pltpu.VMEM((ROUNDS, 8, cx * cy), f32),
                pltpu.VMEM((ROUNDS, 2, cy, cz), f32),
                pltpu.VMEM((ROUNDS, 2, cx, cz), f32),
                pltpu.VMEM((ROUNDS, 2, 8, cx * cy), f32),
                pltpu.VMEM((8, cz), f32),
                pltpu.VMEM((devices, 8, cz), f32),
                pltpu.VMEM((nx * (cx // 4), rows, wide), f32),
                pltpu.VMEM((nx * (cx // 4), rows, wide), f32),
                pltpu.VMEM((nx * (cx // 4) + 2, rows, wide), f32),
                pltpu.SemaphoreType.DMA((ROUNDS, 6)),
                pltpu.SemaphoreType.DMA((ROUNDS, 6)),
                pltpu.SemaphoreType.DMA((devices,)),
                pltpu.SemaphoreType.DMA((devices,)),
            ],
            compiler_params=pltpu.CompilerParams(
                collective_id=0, has_side_effects=True, vmem_limit_bytes=60 * 1024 * 1024
            ),
        )(divergence, damping, *tables)

    spec = P(*AXES)
    return jax.shard_map(local, mesh=mesh, in_specs=(spec, spec), out_specs=spec, check_vma=False)
```

```python
import functools
import math

import jax
import jax.numpy as jnp
import numpy as np
from jax import lax
from jax.experimental import pallas as pl
from jax.experimental.pallas import tpu as pltpu
from jax.sharding import PartitionSpec as P

AXES = ("gx", "gy", "gz")
ROUNDS = 7
WEIGHT = 2.0 / 3.0
MESH = pl.DeviceIdType.MESH
HIGH = lax.Precision.HIGHEST


def dot(a, b, dims=(((1,), (0,)), ((), ()))):
    return lax.dot_general(a, b, dims, precision=HIGH, preferred_element_type=jnp.float32)


def one_hot(condition):
    return jnp.where(condition, 1.0, 0.0).astype(jnp.float32)


def iota(shape, dim):
    return lax.broadcasted_iota(jnp.int32, shape, dim)


def coarsen_dup(values, step):
    nx, ny, nz = values.shape
    pairs = values.reshape(nx // 2, 2, ny, nz)
    total = pairs[:, 0] + pairs[:, 1]
    for dim, size in ((1, ny), (2, nz)):
        even = (iota(total.shape, dim) // step) % 2 == 0
        total = total + jnp.where(
            even, pltpu.roll(total, size - step, dim), pltpu.roll(total, step, dim)
        )
    return total * 0.125


def expand_x(values, times):
    nx, ny, nz = values.shape
    return jnp.broadcast_to(values[:, None], (nx, times, ny, nz)).reshape(nx * times, ny, nz)


def sum_x(values, low, high):
    return jnp.concatenate([low[None], values[:-1]], 0) + jnp.concatenate(
        [values[1:], high[None]], 0
    )


def neighbours_global(values, step, valid_z):
    nx, ny, nz = values.shape
    zero = jnp.zeros((ny, nz), jnp.float32)
    total = sum_x(values, zero, zero)
    row, lane = iota(values.shape, 1), iota(values.shape, 2)
    total = total + jnp.where(row < step, 0.0, pltpu.roll(values, step, 1))
    total = total + jnp.where(row >= ny - step, 0.0, pltpu.roll(values, ny - step, 1))
    total = total + jnp.where(lane < step, 0.0, pltpu.roll(values, step, 2))
    total = total + jnp.where(lane >= valid_z - step, 0.0, pltpu.roll(values, nz - step, 2))
    return total


def kernel(
    counts, tables, b_ref, d_ref, ty_ref, tz_ref, den_ref, out_ref,
    xsend, ysend, zsend, xrecv, yrecv, zrecv, pay, gathered, gb, gd, v2,
    ssem, rsem, gssem, grsem,
):
    cx, cy, cz = counts
    table_x = tables
    nx, ny, nz = (lax.axis_size(a) for a in AXES)
    devices = nx * ny * nz
    gx, gy, gz = (lax.axis_index(a) for a in AXES)
    place = {"gx": gx, "gy": gy, "gz": gz}
    size = {"gx": nx, "gy": ny, "gz": nz}
    me = (gx * ny + gy) * nz + gz

    def shifted(position, by, count):
        moved = position + by
        return jnp.where(moved >= count, moved - count, moved)

    along = {a: [shifted(place[a], k, size[a]) for k in range(size[a])] for a in AXES}
    offsets = [(i, j, k) for i in range(nx) for j in range(ny) for k in range(nz)][1:]
    offsets.sort(key=lambda o: -sum(min(d, n - d) for d, n in zip(o, (nx, ny, nz))))

    def peer(offset):
        return tuple(along[a][d] for a, d in zip(AXES, offset))

    def coords(index):
        return (index // (ny * nz), (index // nz) % ny, index % nz)

    def for_peers(act):
        if devices <= 64:
            for number, offset in enumerate(offsets):
                act(number, peer(offset), peer(tuple(-d % n for d, n in zip(offset, (nx, ny, nz)))))
        else:

            @pl.loop(1, devices)
            def _(k):
                act(k, coords((me + k) % devices), coords((me + devices - k) % devices))

    xrecv[...] = jnp.zeros_like(xrecv)
    yrecv[...] = jnp.zeros_like(yrecv)
    zrecv[...] = jnp.zeros_like(zrecv)

    barrier = pltpu.get_barrier_semaphore()

    for_peers(lambda _, to, back: pl.semaphore_signal(barrier, 1, device_id=to, device_id_type=MESH))

    b0 = b_ref[...]
    d0 = d_ref[...]

    def copies(r, level_x):
        result = []
        for axis_number, (axis, send, recv, length) in enumerate(
            (("gx", xsend, xrecv, cy), ("gy", ysend, yrecv, level_x), ("gz", zsend, zrecv, cy))
        ):
            for side in (0, 1):
                other = 1 - side
                index = 2 * axis_number
                cut = pl.ds(0, length)
                src = send.at[r, cut] if axis == "gz" else send.at[r, side, cut]
                target = dict(place)
                target[axis] = place[axis] + (1 if side else -1)
                device = tuple(target[a] for a in AXES)
                exists = place[axis] < size[axis] - 1 if side else place[axis] > 0
                sent = ssem.at[r, index + side]
                out = functools.partial(
                    pltpu.make_async_remote_copy,
                    src, recv.at[r, other, cut], sent, rsem.at[r, index + other], device, MESH,
                )
                back = functools.partial(
                    pltpu.make_async_remote_copy,
                    src, recv.at[r, side, cut], sent, rsem.at[r, index + side], device, MESH,
                )
                result.append((exists, out, back))
        return result

    def pack(r, values, step):
        level_x = values.shape[0]
        xsend[r, 0] = values[0]
        xsend[r, 1] = values[-1]
        ysend[r, 0, 0:level_x] = values[:, 0, :]
        ysend[r, 1, 0:level_x] = values[:, cy - 1, :]
        lane = iota((cy, cz), 1)
        both = jnp.zeros((cy, cz), jnp.float32)
        for x in range(level_x):
            both = jnp.where(
                lane // (2 * step) == x, pltpu.roll(values[x], 2 * step * x + step, 1), both
            )
        zsend[r] = both

    def send(r, level_x):
        for exists, out, _ in copies(r, level_x):
            pl.when(exists)(lambda: out().start())

    def exchange(r, values, step):
        pack(r, values, step)
        send(r, values.shape[0])

    def neighbours(r, values, step):
        level_x = values.shape[0]
        row, lane = iota(values.shape, 1), iota(values.shape, 2)
        before, after = pltpu.roll(values, step, 2), pltpu.roll(values, cz - step, 2)
        up, down = pltpu.roll(values, step, 1), pltpu.roll(values, cy - step, 1)
        for exists, _, back in copies(r, level_x):
            pl.when(exists)(lambda: back().wait_recv())
        flat_lane = iota((cy, cz), 1)
        both = jnp.where(
            (flat_lane // step) % 2 == 0,
            pltpu.roll(zrecv[r, 1], cz - step, 1),
            pltpu.roll(zrecv[r, 0], step, 1),
        )
        edge = jnp.stack(
            [pltpu.roll(both, cz - 2 * step * x - step, 1) for x in range(level_x)]
        )
        total = jnp.where(lane < step, edge, before)
        total = total + jnp.where(lane >= cz - step, edge, after)
        total = total + sum_x(values, xrecv[r, 0], xrecv[r, 1])
        low, high = yrecv[r, 0, 0:level_x], yrecv[r, 1, 0:level_x]
        total = total + jnp.where(row < step, low[:, None, :], up)
        total = total + jnp.where(row >= cy - step, high[:, None, :], down)
        return total

    def sweep(values, around, source, scaled, coupling):
        return values * (1.0 - WEIGHT) + scaled * (source + coupling * around)

    diag0 = 6.0 + d0
    scaled0 = WEIGHT / diag0
    v = scaled0 * b0
    pack(0, v, 1)
    d1 = coarsen_dup(d0, 1)
    d2 = coarsen_dup(d1, 2)
    pl.semaphore_wait(barrier, devices - 1)
    send(0, cx)
    s0 = sweep(v, neighbours(0, v, 1), b0, scaled0, 1.0)
    exchange(1, s0, 1)
    b1 = coarsen_dup(b0 - diag0 * s0 + neighbours(1, s0, 1), 1)

    diag1 = 1.5 + d1
    scaled1 = WEIGHT / diag1
    v = scaled1 * b1
    exchange(2, v, 2)
    s1 = sweep(v, neighbours(2, v, 2), b1, scaled1, 0.25)
    exchange(3, s1, 2)
    around1 = neighbours(3, s1, 2)
    b2 = coarsen_dup(b1 - diag1 * s1 + 0.25 * around1, 2)

    qx, qy, qz = cx // 4, cy // 4, cz // 4
    row, lane = iota((cz, cz), 0), iota((cz, cz), 1)
    for which, block in enumerate((b2, d2)):
        flat = jnp.zeros((cy, cz), jnp.float32)
        for x in range(qx):
            place_z = one_hot((lane // qz == x) & (row == 4 * (lane % qz)))
            flat = flat + dot(block[x], place_z)
        pick_y = one_hot(iota((8, cy), 1) == 4 * (iota((8, cy), 0) - which * qy))
        if which:
            pay[...] = packed + dot(pick_y * one_hot(iota((8, cy), 0) >= qy), flat)
        else:
            packed = dot(pick_y * one_hot(iota((8, cy), 0) < qy), flat)
    gathered[me] = pay[...]

    def gather_copy(number, to):
        return pltpu.make_async_remote_copy(
            pay, gathered.at[me], gssem.at[number], grsem.at[me], to, MESH
        )

    def gather_wait(number, to, back):
        origin = (back[0] * ny + back[1]) * nz + back[2]
        pltpu.make_async_remote_copy(
            pay, gathered.at[origin], gssem.at[number], grsem.at[origin], to, MESH
        ).wait_recv()

    for_peers(lambda number, to, back: gather_copy(number, to).start())
    for_peers(gather_wait)

    wide = gb.shape[2]
    valid = nz * qz
    per_tile = cz // qz
    blocks = gathered[...].reshape(nx, ny, nz, 8, cz)
    lane = iota((nx, ny, 8, cz), 3)
    for tile in range(wide // cz):
        for x in range(qx):
            total = jnp.zeros((nx, ny, 8, cz), jnp.float32)
            for spot in range(min(per_tile, nz - tile * per_tile)):
                shift = (qz * (spot - x)) % cz
                piece = blocks[:, :, tile * per_tile + spot]
                if shift:
                    piece = pltpu.roll(piece.reshape(nx * ny * 8, cz), shift, 1).reshape(
                        nx, ny, 8, cz
                    )
                total = jnp.where(lane // qz == spot, piece, total)
            for i in range(nx):
                for j in range(ny):
                    where = (qx * i + x, slice(qy * j, qy * j + qy), slice(tile * cz, tile * cz + cz))
                    gb[where] = total[i, j, 0:qy]
                    gd[where] = total[i, j, qy : 2 * qy]
    b2 = gb[...]
    d2 = gd[...]
    damping_mean = jnp.sum(jnp.sum(d2, 0, keepdims=True), axis=(1, 2), keepdims=True)[0] * (
        1.0 / (b2.shape[0] * b2.shape[1] * valid)
    )
    c2, c3 = 0.25**2, 0.25**3
    diag2 = 6.0 * c2 + d2
    scaled2 = WEIGHT / diag2
    v = scaled2 * b2
    s2 = sweep(v, neighbours_global(v, 1, valid), b2, scaled2, c2)
    near2 = neighbours_global(s2, 1, valid)
    b3 = coarsen_dup(b2 - diag2 * s2 + c2 * near2, 1)
    diag3 = 6.0 * c3 + coarsen_dup(d2, 1)
    scaled3 = WEIGHT / diag3
    v = scaled3 * b3
    s3 = sweep(v, neighbours_global(v, 2, valid), b3, scaled3, c3)
    near3 = neighbours_global(s3, 2, valid)
    rem = b3 - diag3 * s3 + c3 * near3

    bx = cx // 8
    rows = rem.shape[1]
    ty, tz = ty_ref[...], tz_ref[...]
    rem = rem.reshape(nx, bx, rows, wide)
    means = rem[:, 0]
    for i in range(1, bx):
        means = means + rem[:, i]
    means = dot(means.reshape(nx * rows, wide), tz).reshape(nx, rows, wide)
    means = [dot(ty, means[i]) for i in range(nx)]
    spectrum = []
    for a in range(nx):
        term = means[0] * float(table_x[a, 0] / bx)
        for i in range(1, nx):
            term = term + means[i] * float(table_x[a, i] / bx)
        spectrum.append(dot(ty, term / (den_ref[a] + damping_mean)))
    solved = []
    for i in range(nx):
        term = spectrum[0] * float(table_x[i, 0])
        for a in range(1, nx):
            term = term + spectrum[a] * float(table_x[i, a])
        solved.append(term)
    solved = dot(jnp.stack(solved).reshape(nx * rows, wide), tz).reshape(nx, rows, wide)

    v = s3 + expand_x(solved, bx)
    for _ in range(2):
        v = sweep(v, neighbours_global(v, 2, valid), b3, scaled3, c3)
    v = s2 + expand_x(v, 2)
    for _ in range(2):
        v = sweep(v, neighbours_global(v, 1, valid), b2, scaled2, c2)

    zero = jnp.zeros((1, rows, wide), jnp.float32)
    v2[0:1] = zero
    v2[pl.ds(1, qx * nx)] = v
    v2[pl.ds(1 + qx * nx, 1)] = zero
    part = v2[pl.ds(qx * gx, qx + 2)]
    k, at = iota((wide, cz), 0), iota((wide, cz), 1)
    inside = k < valid
    fine = at // 2 + gz * (cz // 2)
    own_z = one_hot(inside & (k == fine // 2))
    next_z = one_hot(inside & (k == (fine + 1) // 2)) + one_hot(
        inside & (k == (fine + 1) // 2 - 1)
    )
    at, k = iota((cy, rows), 0), iota((cy, rows), 1)
    fine = at // 2 + gy * (cy // 2)
    own_y = one_hot(k == fine // 2)
    next_y = one_hot(k == (fine + 1) // 2) + one_hot(k == (fine + 1) // 2 - 1)
    in_z = dot(part.reshape((qx + 2) * rows, wide), own_z).reshape(qx + 2, rows, cz)
    by_z = dot(part[1 : qx + 1].reshape(qx * rows, wide), next_z).reshape(qx, rows, cz)
    own = [dot(own_y, in_z[i]) for i in range(qx + 2)]
    side = [dot(next_y, in_z[i + 1]) + dot(own_y, by_z[i]) for i in range(qx)]
    correction = expand_x(jnp.stack(own[1:-1]), 2)
    near = expand_x(jnp.stack(side), 2) + sum_x(correction, own[0], own[-1])
    v = sweep(s1 + correction, around1 + near, b1, scaled1, 0.25)
    exchange(4, v, 2)
    v = sweep(v, neighbours(4, v, 2), b1, scaled1, 0.25)

    v = s0 + expand_x(v, 2)
    exchange(5, v, 1)
    v = sweep(v, neighbours(5, v, 1), b0, scaled0, 1.0)
    exchange(6, v, 1)
    out_ref[...] = sweep(v, neighbours(6, v, 1), b0, scaled0, 1.0)

    for r in range(ROUNDS):
        for exists, out, _ in copies(r, cx // 2 if r in (2, 3, 4) else cx):
            pl.when(exists)(lambda: out().wait_send())

    for_peers(lambda number, to, back: gather_copy(number, to).wait_send())


def sine_table(points):
    index = np.arange(1, points + 1)
    return math.sqrt(2.0 / (points + 1)) * np.sin(
        math.pi * index[:, None] * index[None, :] / (points + 1)
    )


def eigen_values(points, spacing):
    index = np.arange(1, points + 1)
    return (2.0 - 2.0 * np.cos(math.pi * index / (points + 1))) / (spacing * spacing)


def solution(mesh):
    nx, ny, nz = (mesh.shape[a] for a in AXES)

    def local(divergence, damping):
        cx, cy, cz = divergence.shape
        rows, valid = ny * (cy // 4), nz * (cz // 4)
        wide = -(-valid // cz) * cz
        spread_y, spread_z = cy // 4, cz // 4
        table_y = np.repeat(np.repeat(sine_table(ny), spread_y, 0), spread_y, 1) / spread_y
        table_z = np.zeros((wide, wide))
        table_z[:valid, :valid] = (
            np.repeat(np.repeat(sine_table(nz), spread_z, 0), spread_z, 1) / spread_z
        )
        den = np.ones((nx, rows, wide))
        den[:, :, :valid] = (
            eigen_values(nx, cx)[:, None, None]
            + np.repeat(eigen_values(ny, cy), spread_y)[None, :, None]
            + np.repeat(eigen_values(nz, cz), spread_z)[None, None, :]
        )
        tables = [jnp.asarray(t, jnp.float32) for t in (table_y, table_z, den)]
        f32 = jnp.float32
        devices = nx * ny * nz
        return pl.pallas_call(
            functools.partial(kernel, (cx, cy, cz), sine_table(nx)),
            out_shape=jax.ShapeDtypeStruct(divergence.shape, f32),
            in_specs=[pl.BlockSpec(memory_space=pltpu.VMEM)] * 5,
            out_specs=pl.BlockSpec(memory_space=pltpu.VMEM),
            scratch_shapes=[
                pltpu.VMEM((ROUNDS, 2, cy, cz), f32),
                pltpu.VMEM((ROUNDS, 2, cx, cz), f32),
                pltpu.VMEM((ROUNDS, cy, cz), f32),
                pltpu.VMEM((ROUNDS, 2, cy, cz), f32),
                pltpu.VMEM((ROUNDS, 2, cx, cz), f32),
                pltpu.VMEM((ROUNDS, 2, cy, cz), f32),
                pltpu.VMEM((8, cz), f32),
                pltpu.VMEM((devices, 8, cz), f32),
                pltpu.VMEM((nx * (cx // 4), rows, wide), f32),
                pltpu.VMEM((nx * (cx // 4), rows, wide), f32),
                pltpu.VMEM((nx * (cx // 4) + 2, rows, wide), f32),
                pltpu.SemaphoreType.DMA((ROUNDS, 6)),
                pltpu.SemaphoreType.DMA((ROUNDS, 6)),
                pltpu.SemaphoreType.DMA((devices,)),
                pltpu.SemaphoreType.DMA((devices,)),
            ],
            compiler_params=pltpu.CompilerParams(
                collective_id=0, has_side_effects=True, vmem_limit_bytes=60 * 1024 * 1024
            ),
        )(divergence, damping, *tables)

    spec = P(*AXES)
    return jax.shard_map(local, mesh=mesh, in_specs=(spec, spec), out_specs=spec, check_vma=False)
```

```python
import functools
import math

import jax
import jax.numpy as jnp
import numpy as np
from jax import lax
from jax.experimental import pallas as pl
from jax.experimental.pallas import tpu as pltpu
from jax.sharding import PartitionSpec as P

AXES = ("gx", "gy", "gz")
ROUNDS = 8
WEIGHT = 2.0 / 3.0
MESH = pl.DeviceIdType.MESH
HIGH = lax.Precision.HIGHEST


def dot(a, b, dims=(((1,), (0,)), ((), ()))):
    return lax.dot_general(a, b, dims, precision=HIGH, preferred_element_type=jnp.float32)


def one_hot(condition):
    return jnp.where(condition, 1.0, 0.0).astype(jnp.float32)


def iota(shape, dim):
    return lax.broadcasted_iota(jnp.int32, shape, dim)


def coarsen_dup(values, step):
    nx, ny, nz = values.shape
    pairs = values.reshape(nx // 2, 2, ny, nz)
    total = pairs[:, 0] + pairs[:, 1]
    for dim, size in ((1, ny), (2, nz)):
        even = (iota(total.shape, dim) // step) % 2 == 0
        total = total + jnp.where(
            even, pltpu.roll(total, size - step, dim), pltpu.roll(total, step, dim)
        )
    return total * 0.125


def expand_x(values, times):
    nx, ny, nz = values.shape
    return jnp.broadcast_to(values[:, None], (nx, times, ny, nz)).reshape(nx * times, ny, nz)


def sum_x(values, low, high):
    return jnp.concatenate([low[None], values[:-1]], 0) + jnp.concatenate(
        [values[1:], high[None]], 0
    )


def neighbours_global(values, step, valid_z):
    nx, ny, nz = values.shape
    zero = jnp.zeros((ny, nz), jnp.float32)
    total = sum_x(values, zero, zero)
    row, lane = iota(values.shape, 1), iota(values.shape, 2)
    total = total + jnp.where(row < step, 0.0, pltpu.roll(values, step, 1))
    total = total + jnp.where(row >= ny - step, 0.0, pltpu.roll(values, ny - step, 1))
    total = total + jnp.where(lane < step, 0.0, pltpu.roll(values, step, 2))
    total = total + jnp.where(lane >= valid_z - step, 0.0, pltpu.roll(values, nz - step, 2))
    return total


def kernel(
    counts, tables, b_ref, d_ref, ty_ref, tz_ref, den_ref, out_ref,
    xsend, ysend, zsend, xrecv, yrecv, zrecv, pay, gathered, gb, gd, v2,
    ssem, rsem, gssem, grsem,
):
    cx, cy, cz = counts
    table_x = tables
    nx, ny, nz = (lax.axis_size(a) for a in AXES)
    devices = nx * ny * nz
    gx, gy, gz = (lax.axis_index(a) for a in AXES)
    place = {"gx": gx, "gy": gy, "gz": gz}
    size = {"gx": nx, "gy": ny, "gz": nz}
    me = (gx * ny + gy) * nz + gz

    def shifted(position, by, count):
        moved = position + by
        return jnp.where(moved >= count, moved - count, moved)

    along = {a: [shifted(place[a], k, size[a]) for k in range(size[a])] for a in AXES}
    offsets = [(i, j, k) for i in range(nx) for j in range(ny) for k in range(nz)][1:]
    offsets.sort(key=lambda o: -sum(min(d, n - d) for d, n in zip(o, (nx, ny, nz))))

    def peer(offset):
        return tuple(along[a][d] for a, d in zip(AXES, offset))

    def coords(index):
        return (index // (ny * nz), (index // nz) % ny, index % nz)

    def for_peers(act):
        if devices <= 64:
            for number, offset in enumerate(offsets):
                act(number, peer(offset), peer(tuple(-d % n for d, n in zip(offset, (nx, ny, nz)))))
        else:

            @pl.loop(1, devices)
            def _(k):
                act(k, coords((me + k) % devices), coords((me + devices - k) % devices))

    xrecv[...] = jnp.zeros_like(xrecv)
    yrecv[...] = jnp.zeros_like(yrecv)
    zrecv[...] = jnp.zeros_like(zrecv)

    barrier = pltpu.get_barrier_semaphore()

    for_peers(lambda _, to, back: pl.semaphore_signal(barrier, 1, device_id=to, device_id_type=MESH))

    b0 = b_ref[...]
    d0 = d_ref[...]

    def copies(r, level_x):
        result = []
        for axis_number, (axis, send, recv, length) in enumerate(
            (("gx", xsend, xrecv, cy), ("gy", ysend, yrecv, level_x), ("gz", zsend, zrecv, cy))
        ):
            for side in (0, 1):
                other = 1 - side
                index = 2 * axis_number
                cut = pl.ds(0, length)
                src = send.at[r, cut] if axis == "gz" else send.at[r, side, cut]
                target = dict(place)
                target[axis] = place[axis] + (1 if side else -1)
                device = tuple(target[a] for a in AXES)
                exists = place[axis] < size[axis] - 1 if side else place[axis] > 0
                sent = ssem.at[r, index + side]
                out = functools.partial(
                    pltpu.make_async_remote_copy,
                    src, recv.at[r, other, cut], sent, rsem.at[r, index + other], device, MESH,
                )
                back = functools.partial(
                    pltpu.make_async_remote_copy,
                    src, recv.at[r, side, cut], sent, rsem.at[r, index + side], device, MESH,
                )
                result.append((exists, out, back))
        return result

    def pack(r, values, step):
        level_x = values.shape[0]
        xsend[r, 0] = values[0]
        xsend[r, 1] = values[-1]
        ysend[r, 0, 0:level_x] = values[:, 0, :]
        ysend[r, 1, 0:level_x] = values[:, cy - 1, :]
        lane = iota((cy, cz), 1)
        both = jnp.zeros((cy, cz), jnp.float32)
        for x in range(level_x):
            both = jnp.where(
                lane // (2 * step) == x, pltpu.roll(values[x], 2 * step * x + step, 1), both
            )
        zsend[r] = both

    def send(r, level_x):
        for exists, out, _ in copies(r, level_x):
            pl.when(exists)(lambda: out().start())

    def exchange(r, values, step):
        pack(r, values, step)
        send(r, values.shape[0])

    def receive(r, level_x, step):
        for exists, _, back in copies(r, level_x):
            pl.when(exists)(lambda: back().wait_recv())
        flat_lane = iota((cy, cz), 1)
        both = jnp.where(
            (flat_lane // step) % 2 == 0,
            pltpu.roll(zrecv[r, 1], cz - step, 1),
            pltpu.roll(zrecv[r, 0], step, 1),
        )
        edge = jnp.stack(
            [pltpu.roll(both, cz - 2 * step * x - step, 1) for x in range(level_x)]
        )
        return (
            xrecv[r, 0], xrecv[r, 1], yrecv[r, 0, 0:level_x], yrecv[r, 1, 0:level_x], edge,
        )

    def inner(values, step):
        return (
            pltpu.roll(values, step, 2), pltpu.roll(values, cz - step, 2),
            pltpu.roll(values, step, 1), pltpu.roll(values, cy - step, 1),
        )

    def add_up(values, rolled, faces, step):
        row, lane = iota(values.shape, 1), iota(values.shape, 2)
        before, after, up, down = rolled
        x_low, x_high, low, high, edge = faces
        total = jnp.where(lane < step, edge, before)
        total = total + jnp.where(lane >= cz - step, edge, after)
        total = total + sum_x(values, x_low, x_high)
        total = total + jnp.where(row < step, low[:, None, :], up)
        total = total + jnp.where(row >= cy - step, high[:, None, :], down)
        return total

    def neighbours(r, values, step):
        rolled = inner(values, step)
        return add_up(values, rolled, receive(r, values.shape[0], step), step)

    def sweep(values, around, source, scaled, coupling):
        return values * (1.0 - WEIGHT) + scaled * (source + coupling * around)

    diag0 = 6.0 + d0
    scaled0 = WEIGHT / diag0
    v = scaled0 * b0
    pack(0, v, 1)
    d1 = coarsen_dup(d0, 1)
    d2 = coarsen_dup(d1, 2)
    pl.semaphore_wait(barrier, devices - 1)
    send(0, cx)
    diag1 = 1.5 + d1
    scaled1 = WEIGHT / diag1
    exchange(4, scaled1, 2)
    s0 = sweep(v, neighbours(0, v, 1), b0, scaled0, 1.0)
    exchange(1, s0, 1)
    b1 = coarsen_dup(b0 - diag0 * s0 + neighbours(1, s0, 1), 1)

    v = scaled1 * b1
    exchange(2, v, 2)
    s1 = sweep(v, neighbours(2, v, 2), b1, scaled1, 0.25)
    exchange(3, s1, 2)
    around1 = neighbours(3, s1, 2)
    b2 = coarsen_dup(b1 - diag1 * s1 + 0.25 * around1, 2)

    qx, qy, qz = cx // 4, cy // 4, cz // 4
    row, lane = iota((cz, cz), 0), iota((cz, cz), 1)
    for which, block in enumerate((b2, d2)):
        flat = jnp.zeros((cy, cz), jnp.float32)
        for x in range(qx):
            place_z = one_hot((lane // qz == x) & (row == 4 * (lane % qz)))
            flat = flat + dot(block[x], place_z)
        pick_y = one_hot(iota((8, cy), 1) == 4 * (iota((8, cy), 0) - which * qy))
        if which:
            pay[...] = packed + dot(pick_y * one_hot(iota((8, cy), 0) >= qy), flat)
        else:
            packed = dot(pick_y * one_hot(iota((8, cy), 0) < qy), flat)
    gathered[me] = pay[...]

    def gather_copy(number, to):
        return pltpu.make_async_remote_copy(
            pay, gathered.at[me], gssem.at[number], grsem.at[me], to, MESH
        )

    def gather_wait(number, to, back):
        origin = (back[0] * ny + back[1]) * nz + back[2]
        pltpu.make_async_remote_copy(
            pay, gathered.at[origin], gssem.at[number], grsem.at[origin], to, MESH
        ).wait_recv()

    for_peers(lambda number, to, back: gather_copy(number, to).start())

    swept1 = sweep(s1, around1, b1, scaled1, 0.25)
    exchange(7, swept1, 2)
    for_peers(gather_wait)

    wide = gb.shape[2]
    valid = nz * qz
    per_tile = cz // qz
    blocks = gathered[...].reshape(nx, ny, nz, 8, cz)
    lane = iota((nx, ny, 8, cz), 3)
    for tile in range(wide // cz):
        for x in range(qx):
            total = jnp.zeros((nx, ny, 8, cz), jnp.float32)
            for spot in range(min(per_tile, nz - tile * per_tile)):
                shift = (qz * (spot - x)) % cz
                piece = blocks[:, :, tile * per_tile + spot]
                if shift:
                    piece = pltpu.roll(piece.reshape(nx * ny * 8, cz), shift, 1).reshape(
                        nx, ny, 8, cz
                    )
                total = jnp.where(lane // qz == spot, piece, total)
            for i in range(nx):
                for j in range(ny):
                    where = (qx * i + x, slice(qy * j, qy * j + qy), slice(tile * cz, tile * cz + cz))
                    gb[where] = total[i, j, 0:qy]
                    gd[where] = total[i, j, qy : 2 * qy]
    b2 = gb[...]
    d2 = gd[...]
    damping_mean = jnp.sum(jnp.sum(d2, 0, keepdims=True), axis=(1, 2), keepdims=True)[0] * (
        1.0 / (b2.shape[0] * b2.shape[1] * valid)
    )
    c2, c3 = 0.25**2, 0.25**3
    diag2 = 6.0 * c2 + d2
    scaled2 = WEIGHT / diag2
    v = scaled2 * b2
    s2 = sweep(v, neighbours_global(v, 1, valid), b2, scaled2, c2)
    near2 = neighbours_global(s2, 1, valid)
    b3 = coarsen_dup(b2 - diag2 * s2 + c2 * near2, 1)
    diag3 = 6.0 * c3 + coarsen_dup(d2, 1)
    scaled3 = WEIGHT / diag3
    v = scaled3 * b3
    s3 = sweep(v, neighbours_global(v, 2, valid), b3, scaled3, c3)
    near3 = neighbours_global(s3, 2, valid)
    rem = b3 - diag3 * s3 + c3 * near3

    bx = cx // 8
    rows = rem.shape[1]
    ty, tz = ty_ref[...], tz_ref[...]
    rem = rem.reshape(nx, bx, rows, wide)
    means = rem[:, 0]
    for i in range(1, bx):
        means = means + rem[:, i]
    means = dot(means.reshape(nx * rows, wide), tz).reshape(nx, rows, wide)
    means = [dot(ty, means[i]) for i in range(nx)]
    spectrum = []
    for a in range(nx):
        term = means[0] * float(table_x[a, 0] / bx)
        for i in range(1, nx):
            term = term + means[i] * float(table_x[a, i] / bx)
        spectrum.append(dot(ty, term / (den_ref[a] + damping_mean)))
    solved = []
    for i in range(nx):
        term = spectrum[0] * float(table_x[i, 0])
        for a in range(1, nx):
            term = term + spectrum[a] * float(table_x[i, a])
        solved.append(term)
    solved = dot(jnp.stack(solved).reshape(nx * rows, wide), tz).reshape(nx, rows, wide)

    v = s3 + expand_x(solved, bx)
    for _ in range(2):
        v = sweep(v, neighbours_global(v, 2, valid), b3, scaled3, c3)
    v = s2 + expand_x(v, 2)
    for _ in range(2):
        v = sweep(v, neighbours_global(v, 1, valid), b2, scaled2, c2)

    zero = jnp.zeros((1, rows, wide), jnp.float32)
    v2[0:1] = zero
    v2[pl.ds(1, qx * nx)] = v
    v2[pl.ds(1 + qx * nx, 1)] = zero
    part = v2[pl.ds(qx * gx, qx + 2)]
    k, at = iota((wide, 2 * cz), 0), iota((wide, 2 * cz), 1)
    inside, first = k < valid, gz * (cz // 2)
    beside = jnp.where(at < cz + 2, first - 1, first + cz // 2)
    fine = jnp.where(at < cz, at // 2 + first, beside)
    inside = inside & ((at < cz + 2) | (at >= 2 * cz - 2))
    own_z = one_hot(inside & (k == (fine >> 1)))
    next_z = one_hot(inside & (k == (fine + 1) >> 1)) + one_hot(
        inside & (k == ((fine + 1) >> 1) - 1)
    )
    at, k = iota((cy + 8, rows), 0), iota((cy + 8, rows), 1)
    first = gy * (cy // 2)
    fine = jnp.where(at < cy, at // 2 + first, jnp.where(at == cy, first - 1, first + cy // 2))
    own_y = one_hot(k == (fine >> 1))
    next_y = one_hot(k == (fine + 1) >> 1) + one_hot(k == ((fine + 1) >> 1) - 1)
    flat = part.reshape((qx + 2) * rows, wide)
    in_z = dot(flat, own_z).reshape(qx + 2, rows, 2 * cz)
    by_z = dot(flat, next_z).reshape(qx + 2, rows, 2 * cz)
    own = jnp.stack([dot(own_y, in_z[i]) for i in range(qx + 2)])
    side = jnp.stack([dot(next_y, in_z[i]) + dot(own_y, by_z[i]) for i in range(qx + 2)])
    own, side = expand_x(own, 2), expand_x(side, 2)
    near = side[1:-1] + own[:-2] + own[2:]
    own = own[1:-1]
    faces, scales = receive(7, cx // 2, 2), receive(4, cx // 2, 2)
    spots = (
        (0, slice(0, cy), slice(0, cz)),
        (-1, slice(0, cy), slice(0, cz)),
        (slice(1, -1), cy, slice(0, cz)),
        (slice(1, -1), cy + 1, slice(0, cz)),
        (slice(1, -1), slice(0, cy), slice(cz, 2 * cz)),
    )

    def swept(base, scaled, spot):
        return base + own[spot] * (1.0 - WEIGHT) + scaled * (0.25 * near[spot])

    v = swept(swept1, scaled1, (slice(1, -1), slice(0, cy), slice(0, cz)))
    faces = [swept(f, g, spot) for f, g, spot in zip(faces, scales, spots)]
    v = sweep(v, add_up(v, inner(v, 2), faces, 2), b1, scaled1, 0.25)

    v = s0 + expand_x(v, 2)
    exchange(5, v, 1)
    v = sweep(v, neighbours(5, v, 1), b0, scaled0, 1.0)
    exchange(6, v, 1)
    out_ref[...] = sweep(v, neighbours(6, v, 1), b0, scaled0, 1.0)

    for r in range(ROUNDS):
        for exists, out, _ in copies(r, cx // 2 if r in (2, 3, 4, 7) else cx):
            pl.when(exists)(lambda: out().wait_send())

    for_peers(lambda number, to, back: gather_copy(number, to).wait_send())


def sine_table(points):
    index = np.arange(1, points + 1)
    return math.sqrt(2.0 / (points + 1)) * np.sin(
        math.pi * index[:, None] * index[None, :] / (points + 1)
    )


def eigen_values(points, spacing):
    index = np.arange(1, points + 1)
    return (2.0 - 2.0 * np.cos(math.pi * index / (points + 1))) / (spacing * spacing)


def solution(mesh):
    nx, ny, nz = (mesh.shape[a] for a in AXES)

    def local(divergence, damping):
        cx, cy, cz = divergence.shape
        rows, valid = ny * (cy // 4), nz * (cz // 4)
        wide = -(-valid // cz) * cz
        spread_y, spread_z = cy // 4, cz // 4
        table_y = np.repeat(np.repeat(sine_table(ny), spread_y, 0), spread_y, 1) / spread_y
        table_z = np.zeros((wide, wide))
        table_z[:valid, :valid] = (
            np.repeat(np.repeat(sine_table(nz), spread_z, 0), spread_z, 1) / spread_z
        )
        den = np.ones((nx, rows, wide))
        den[:, :, :valid] = (
            eigen_values(nx, cx)[:, None, None]
            + np.repeat(eigen_values(ny, cy), spread_y)[None, :, None]
            + np.repeat(eigen_values(nz, cz), spread_z)[None, None, :]
        )
        tables = [jnp.asarray(t, jnp.float32) for t in (table_y, table_z, den)]
        f32 = jnp.float32
        devices = nx * ny * nz
        return pl.pallas_call(
            functools.partial(kernel, (cx, cy, cz), sine_table(nx)),
            out_shape=jax.ShapeDtypeStruct(divergence.shape, f32),
            in_specs=[pl.BlockSpec(memory_space=pltpu.VMEM)] * 5,
            out_specs=pl.BlockSpec(memory_space=pltpu.VMEM),
            scratch_shapes=[
                pltpu.VMEM((ROUNDS, 2, cy, cz), f32),
                pltpu.VMEM((ROUNDS, 2, cx, cz), f32),
                pltpu.VMEM((ROUNDS, cy, cz), f32),
                pltpu.VMEM((ROUNDS, 2, cy, cz), f32),
                pltpu.VMEM((ROUNDS, 2, cx, cz), f32),
                pltpu.VMEM((ROUNDS, 2, cy, cz), f32),
                pltpu.VMEM((8, cz), f32),
                pltpu.VMEM((devices, 8, cz), f32),
                pltpu.VMEM((nx * (cx // 4), rows, wide), f32),
                pltpu.VMEM((nx * (cx // 4), rows, wide), f32),
                pltpu.VMEM((nx * (cx // 4) + 2, rows, wide), f32),
                pltpu.SemaphoreType.DMA((ROUNDS, 6)),
                pltpu.SemaphoreType.DMA((ROUNDS, 6)),
                pltpu.SemaphoreType.DMA((devices,)),
                pltpu.SemaphoreType.DMA((devices,)),
            ],
            compiler_params=pltpu.CompilerParams(
                collective_id=0, has_side_effects=True, vmem_limit_bytes=60 * 1024 * 1024
            ),
        )(divergence, damping, *tables)

    spec = P(*AXES)
    return jax.shard_map(local, mesh=mesh, in_specs=(spec, spec), out_specs=spec, check_vma=False)
```

```python
import functools
import math

import jax
import jax.numpy as jnp
import numpy as np
from jax import lax
from jax.experimental import pallas as pl
from jax.experimental.pallas import tpu as pltpu
from jax.sharding import PartitionSpec as P

AXES = ("gx", "gy", "gz")
ROUNDS = 8
WEIGHT = 2.0 / 3.0
MESH = pl.DeviceIdType.MESH
HIGH = lax.Precision.HIGHEST


def dot(a, b, dims=(((1,), (0,)), ((), ()))):
    return lax.dot_general(a, b, dims, precision=HIGH, preferred_element_type=jnp.float32)


def one_hot(condition):
    return jnp.where(condition, 1.0, 0.0).astype(jnp.float32)


def iota(shape, dim):
    return lax.broadcasted_iota(jnp.int32, shape, dim)


def coarsen_dup(values, step):
    nx, ny, nz = values.shape
    pairs = values.reshape(nx // 2, 2, ny, nz)
    total = pairs[:, 0] + pairs[:, 1]
    for dim, size in ((1, ny), (2, nz)):
        even = (iota(total.shape, dim) // step) % 2 == 0
        total = total + jnp.where(
            even, pltpu.roll(total, size - step, dim), pltpu.roll(total, step, dim)
        )
    return total * 0.125


def expand_x(values, times):
    nx, ny, nz = values.shape
    return jnp.broadcast_to(values[:, None], (nx, times, ny, nz)).reshape(nx * times, ny, nz)


def sum_x(values, low, high):
    return jnp.concatenate([low[None], values[:-1]], 0) + jnp.concatenate(
        [values[1:], high[None]], 0
    )


def neighbours_global(values, step, valid_z):
    nx, ny, nz = values.shape
    zero = jnp.zeros((ny, nz), jnp.float32)
    total = sum_x(values, zero, zero)
    row, lane = iota(values.shape, 1), iota(values.shape, 2)
    total = total + jnp.where(row < step, 0.0, pltpu.roll(values, step, 1))
    total = total + jnp.where(row >= ny - step, 0.0, pltpu.roll(values, ny - step, 1))
    total = total + jnp.where(lane < step, 0.0, pltpu.roll(values, step, 2))
    total = total + jnp.where(lane >= valid_z - step, 0.0, pltpu.roll(values, nz - step, 2))
    return total


def kernel(
    counts, tables, b_ref, d_ref, ty_ref, tz_ref, den_ref, out_ref,
    xsend, ysend, zsend, xrecv, yrecv, zrecv, pay, gathered, joined, gb, gd, v2,
    ssem, rsem, gssem, grsem,
):
    cx, cy, cz = counts
    table_x = tables
    nx, ny, nz = (lax.axis_size(a) for a in AXES)
    devices = nx * ny * nz
    gx, gy, gz = (lax.axis_index(a) for a in AXES)
    place = {"gx": gx, "gy": gy, "gz": gz}
    size = {"gx": nx, "gy": ny, "gz": nz}
    me = (gx * ny + gy) * nz + gz

    def shifted(position, by, count):
        moved = position + by
        return jnp.where(moved >= count, moved - count, moved)

    along = {a: [shifted(place[a], k, size[a]) for k in range(size[a])] for a in AXES}
    offsets = [(i, j, k) for i in range(nx) for j in range(ny) for k in range(nz)][1:]
    offsets.sort(key=lambda o: -sum(min(d, n - d) for d, n in zip(o, (nx, ny, nz))))

    def peer(offset):
        return tuple(along[a][d] for a, d in zip(AXES, offset))

    def coords(index):
        return (index // (ny * nz), (index // nz) % ny, index % nz)

    def for_peers(act):
        if devices <= 64:
            for number, offset in enumerate(offsets):
                act(number, peer(offset), peer(tuple(-d % n for d, n in zip(offset, (nx, ny, nz)))))
        else:

            @pl.loop(1, devices)
            def _(k):
                act(k, coords((me + k) % devices), coords((me + devices - k) % devices))

    xrecv[...] = jnp.zeros_like(xrecv)
    yrecv[...] = jnp.zeros_like(yrecv)
    zrecv[...] = jnp.zeros_like(zrecv)

    barrier = pltpu.get_barrier_semaphore()

    for_peers(lambda _, to, back: pl.semaphore_signal(barrier, 1, device_id=to, device_id_type=MESH))

    b0 = b_ref[...]
    d0 = d_ref[...]

    def copies(r, level_x):
        result = []
        for axis_number, (axis, send, recv, length) in enumerate(
            (("gx", xsend, xrecv, cy), ("gy", ysend, yrecv, level_x), ("gz", zsend, zrecv, cy))
        ):
            for side in (0, 1):
                other = 1 - side
                index = 2 * axis_number
                cut = pl.ds(0, length)
                src = send.at[r, cut] if axis == "gz" else send.at[r, side, cut]
                target = dict(place)
                target[axis] = place[axis] + (1 if side else -1)
                device = tuple(target[a] for a in AXES)
                exists = place[axis] < size[axis] - 1 if side else place[axis] > 0
                sent = ssem.at[r, index + side]
                out = functools.partial(
                    pltpu.make_async_remote_copy,
                    src, recv.at[r, other, cut], sent, rsem.at[r, index + other], device, MESH,
                )
                back = functools.partial(
                    pltpu.make_async_remote_copy,
                    src, recv.at[r, side, cut], sent, rsem.at[r, index + side], device, MESH,
                )
                result.append((exists, out, back))
        return result

    def pack(r, values, step):
        level_x = values.shape[0]
        xsend[r, 0] = values[0]
        xsend[r, 1] = values[-1]
        ysend[r, 0, 0:level_x] = values[:, 0, :]
        ysend[r, 1, 0:level_x] = values[:, cy - 1, :]
        lane = iota((cy, cz), 1)
        both = jnp.zeros((cy, cz), jnp.float32)
        for x in range(level_x):
            both = jnp.where(
                lane // (2 * step) == x, pltpu.roll(values[x], 2 * step * x + step, 1), both
            )
        zsend[r] = both

    def send(r, level_x):
        for exists, out, _ in copies(r, level_x):
            pl.when(exists)(lambda: out().start())

    def exchange(r, values, step):
        pack(r, values, step)
        send(r, values.shape[0])

    def receive(r, level_x, step):
        for exists, _, back in copies(r, level_x):
            pl.when(exists)(lambda: back().wait_recv())
        flat_lane = iota((cy, cz), 1)
        both = jnp.where(
            (flat_lane // step) % 2 == 0,
            pltpu.roll(zrecv[r, 1], cz - step, 1),
            pltpu.roll(zrecv[r, 0], step, 1),
        )
        edge = jnp.stack(
            [pltpu.roll(both, cz - 2 * step * x - step, 1) for x in range(level_x)]
        )
        return (
            xrecv[r, 0], xrecv[r, 1], yrecv[r, 0, 0:level_x], yrecv[r, 1, 0:level_x], edge,
        )

    def inner(values, step):
        return (
            pltpu.roll(values, step, 2), pltpu.roll(values, cz - step, 2),
            pltpu.roll(values, step, 1), pltpu.roll(values, cy - step, 1),
        )

    def add_up(values, rolled, faces, step):
        row, lane = iota(values.shape, 1), iota(values.shape, 2)
        before, after, up, down = rolled
        x_low, x_high, low, high, edge = faces
        total = jnp.where(lane < step, edge, before)
        total = total + jnp.where(lane >= cz - step, edge, after)
        total = total + sum_x(values, x_low, x_high)
        total = total + jnp.where(row < step, low[:, None, :], up)
        total = total + jnp.where(row >= cy - step, high[:, None, :], down)
        return total

    def neighbours(r, values, step):
        rolled = inner(values, step)
        return add_up(values, rolled, receive(r, values.shape[0], step), step)

    def sweep(values, around, source, scaled, coupling):
        return values * (1.0 - WEIGHT) + scaled * (source + coupling * around)

    qx, qy, qz = cx // 4, cy // 4, cz // 4

    def flatten(which, block):
        row, lane = iota((cz, cz), 0), iota((cz, cz), 1)
        flat = jnp.zeros((cy, cz), jnp.float32)
        for x in range(qx):
            place_z = one_hot((lane // qz == x) & (row == 4 * (lane % qz)))
            flat = flat + dot(block[x], place_z)
        pick_y = one_hot(iota((8, cy), 1) == 4 * iota((8, cy), 0))
        pay[which] = dot(pick_y, flat)[0:qy]
        gathered[which, me] = pay[which]

    def gather_copy(which, number, to):
        return pltpu.make_async_remote_copy(
            pay.at[which], gathered.at[which, me],
            gssem.at[number], grsem.at[which, me], to, MESH,
        )

    def gather_wait(which, number, to, back):
        origin = (back[0] * ny + back[1]) * nz + back[2]
        pltpu.make_async_remote_copy(
            pay.at[which], gathered.at[which, origin],
            gssem.at[number], grsem.at[which, origin], to, MESH,
        ).wait_recv()

    def sent(r):
        for exists, out, _ in copies(r, cx // 2 if r in (2, 3, 4, 7) else cx):
            pl.when(exists)(lambda: out().wait_send())

    diag0 = 6.0 + d0
    scaled0 = WEIGHT / diag0
    v = scaled0 * b0
    pack(0, v, 1)
    d1 = coarsen_dup(d0, 1)
    d2 = coarsen_dup(d1, 2)
    diag1 = 1.5 + d1
    scaled1 = WEIGHT / diag1
    pack(4, scaled1, 2)
    flatten(1, d2)
    pl.semaphore_wait(barrier, devices - 1)
    send(0, cx)
    send(4, cx // 2)
    for_peers(lambda number, to, back: gather_copy(1, number, to).start())
    s0 = sweep(v, neighbours(0, v, 1), b0, scaled0, 1.0)
    exchange(1, s0, 1)
    b1 = coarsen_dup(b0 - diag0 * s0 + neighbours(1, s0, 1), 1)

    v = scaled1 * b1
    exchange(2, v, 2)
    s1 = sweep(v, neighbours(2, v, 2), b1, scaled1, 0.25)
    exchange(3, s1, 2)
    for_peers(lambda number, to, back: gather_copy(1, number, to).wait_send())
    around1 = neighbours(3, s1, 2)
    b2 = coarsen_dup(b1 - diag1 * s1 + 0.25 * around1, 2)

    flatten(0, b2)
    for_peers(lambda number, to, back: gather_copy(0, number, to).start())
    for r in range(5):
        sent(r)

    swept1 = sweep(s1, around1, b1, scaled1, 0.25)
    exchange(7, swept1, 2)
    for_peers(functools.partial(gather_wait, 1))
    for_peers(functools.partial(gather_wait, 0))
    for index in range(devices):
        joined[index, 0:qy] = gathered[0, index]
        joined[index, qy : 2 * qy] = gathered[1, index]

    wide = gb.shape[2]
    valid = nz * qz
    per_tile = cz // qz
    blocks = joined[...].reshape(nx, ny, nz, 8, cz)
    lane = iota((nx, ny, 8, cz), 3)
    for tile in range(wide // cz):
        for x in range(qx):
            total = jnp.zeros((nx, ny, 8, cz), jnp.float32)
            for spot in range(min(per_tile, nz - tile * per_tile)):
                shift = (qz * (spot - x)) % cz
                piece = blocks[:, :, tile * per_tile + spot]
                if shift:
                    piece = pltpu.roll(piece.reshape(nx * ny * 8, cz), shift, 1).reshape(
                        nx, ny, 8, cz
                    )
                total = jnp.where(lane // qz == spot, piece, total)
            for i in range(nx):
                for j in range(ny):
                    where = (qx * i + x, slice(qy * j, qy * j + qy), slice(tile * cz, tile * cz + cz))
                    gb[where] = total[i, j, 0:qy]
                    gd[where] = total[i, j, qy : 2 * qy]
    b2 = gb[...]
    d2 = gd[...]
    damping_mean = jnp.sum(jnp.sum(d2, 0, keepdims=True), axis=(1, 2), keepdims=True)[0] * (
        1.0 / (b2.shape[0] * b2.shape[1] * valid)
    )
    c2, c3 = 0.25**2, 0.25**3
    diag2 = 6.0 * c2 + d2
    scaled2 = WEIGHT / diag2
    v = scaled2 * b2
    s2 = sweep(v, neighbours_global(v, 1, valid), b2, scaled2, c2)
    near2 = neighbours_global(s2, 1, valid)
    b3 = coarsen_dup(b2 - diag2 * s2 + c2 * near2, 1)
    diag3 = 6.0 * c3 + coarsen_dup(d2, 1)
    scaled3 = WEIGHT / diag3
    v = scaled3 * b3
    s3 = sweep(v, neighbours_global(v, 2, valid), b3, scaled3, c3)
    near3 = neighbours_global(s3, 2, valid)
    rem = b3 - diag3 * s3 + c3 * near3

    bx = cx // 8
    rows = rem.shape[1]
    ty, tz = ty_ref[...], tz_ref[...]
    rem = rem.reshape(nx, bx, rows, wide)
    means = rem[:, 0]
    for i in range(1, bx):
        means = means + rem[:, i]
    means = dot(means.reshape(nx * rows, wide), tz).reshape(nx, rows, wide)
    means = [dot(ty, means[i]) for i in range(nx)]
    spectrum = []
    for a in range(nx):
        term = means[0] * float(table_x[a, 0] / bx)
        for i in range(1, nx):
            term = term + means[i] * float(table_x[a, i] / bx)
        spectrum.append(dot(ty, term / (den_ref[a] + damping_mean)))
    solved = []
    for i in range(nx):
        term = spectrum[0] * float(table_x[i, 0])
        for a in range(1, nx):
            term = term + spectrum[a] * float(table_x[i, a])
        solved.append(term)
    solved = dot(jnp.stack(solved).reshape(nx * rows, wide), tz).reshape(nx, rows, wide)

    v = s3 + expand_x(solved, bx)
    for _ in range(2):
        v = sweep(v, neighbours_global(v, 2, valid), b3, scaled3, c3)
    v = s2 + expand_x(v, 2)
    for _ in range(2):
        v = sweep(v, neighbours_global(v, 1, valid), b2, scaled2, c2)

    zero = jnp.zeros((1, rows, wide), jnp.float32)
    v2[0:1] = zero
    v2[pl.ds(1, qx * nx)] = v
    v2[pl.ds(1 + qx * nx, 1)] = zero
    part = v2[pl.ds(qx * gx, qx + 2)]
    k, at = iota((wide, 2 * cz), 0), iota((wide, 2 * cz), 1)
    inside, first = k < valid, gz * (cz // 2)
    beside = jnp.where(at < cz + 2, first - 1, first + cz // 2)
    fine = jnp.where(at < cz, at // 2 + first, beside)
    inside = inside & ((at < cz + 2) | (at >= 2 * cz - 2))
    own_z = one_hot(inside & (k == (fine >> 1)))
    next_z = one_hot(inside & (k == (fine + 1) >> 1)) + one_hot(
        inside & (k == ((fine + 1) >> 1) - 1)
    )
    at, k = iota((cy + 8, rows), 0), iota((cy + 8, rows), 1)
    first = gy * (cy // 2)
    fine = jnp.where(at < cy, at // 2 + first, jnp.where(at == cy, first - 1, first + cy // 2))
    own_y = one_hot(k == (fine >> 1))
    next_y = one_hot(k == (fine + 1) >> 1) + one_hot(k == ((fine + 1) >> 1) - 1)
    flat = part.reshape((qx + 2) * rows, wide)
    in_z = dot(flat, own_z).reshape(qx + 2, rows, 2 * cz)
    by_z = dot(flat, next_z).reshape(qx + 2, rows, 2 * cz)
    own = jnp.stack([dot(own_y, in_z[i]) for i in range(qx + 2)])
    side = jnp.stack([dot(next_y, in_z[i]) + dot(own_y, by_z[i]) for i in range(qx + 2)])
    own, side = expand_x(own, 2), expand_x(side, 2)
    near = side[1:-1] + own[:-2] + own[2:]
    own = own[1:-1]
    faces, scales = receive(7, cx // 2, 2), receive(4, cx // 2, 2)
    spots = (
        (0, slice(0, cy), slice(0, cz)),
        (-1, slice(0, cy), slice(0, cz)),
        (slice(1, -1), cy, slice(0, cz)),
        (slice(1, -1), cy + 1, slice(0, cz)),
        (slice(1, -1), slice(0, cy), slice(cz, 2 * cz)),
    )

    def swept(base, scaled, spot):
        return base + own[spot] * (1.0 - WEIGHT) + scaled * (0.25 * near[spot])

    v = swept(swept1, scaled1, (slice(1, -1), slice(0, cy), slice(0, cz)))
    faces = [swept(f, g, spot) for f, g, spot in zip(faces, scales, spots)]
    v = sweep(v, add_up(v, inner(v, 2), faces, 2), b1, scaled1, 0.25)

    v = s0 + expand_x(v, 2)
    exchange(5, v, 1)
    for_peers(lambda number, to, back: gather_copy(0, number, to).wait_send())
    sent(7)
    v = sweep(v, neighbours(5, v, 1), b0, scaled0, 1.0)
    exchange(6, v, 1)
    sent(5)
    out_ref[...] = sweep(v, neighbours(6, v, 1), b0, scaled0, 1.0)

    sent(6)


def sine_table(points):
    index = np.arange(1, points + 1)
    return math.sqrt(2.0 / (points + 1)) * np.sin(
        math.pi * index[:, None] * index[None, :] / (points + 1)
    )


def eigen_values(points, spacing):
    index = np.arange(1, points + 1)
    return (2.0 - 2.0 * np.cos(math.pi * index / (points + 1))) / (spacing * spacing)


def solution(mesh):
    nx, ny, nz = (mesh.shape[a] for a in AXES)

    def local(divergence, damping):
        cx, cy, cz = divergence.shape
        rows, valid = ny * (cy // 4), nz * (cz // 4)
        wide = -(-valid // cz) * cz
        spread_y, spread_z = cy // 4, cz // 4
        table_y = np.repeat(np.repeat(sine_table(ny), spread_y, 0), spread_y, 1) / spread_y
        table_z = np.zeros((wide, wide))
        table_z[:valid, :valid] = (
            np.repeat(np.repeat(sine_table(nz), spread_z, 0), spread_z, 1) / spread_z
        )
        den = np.ones((nx, rows, wide))
        den[:, :, :valid] = (
            eigen_values(nx, cx)[:, None, None]
            + np.repeat(eigen_values(ny, cy), spread_y)[None, :, None]
            + np.repeat(eigen_values(nz, cz), spread_z)[None, None, :]
        )
        tables = [jnp.asarray(t, jnp.float32) for t in (table_y, table_z, den)]
        f32 = jnp.float32
        devices = nx * ny * nz
        return pl.pallas_call(
            functools.partial(kernel, (cx, cy, cz), sine_table(nx)),
            out_shape=jax.ShapeDtypeStruct(divergence.shape, f32),
            in_specs=[pl.BlockSpec(memory_space=pltpu.VMEM)] * 5,
            out_specs=pl.BlockSpec(memory_space=pltpu.VMEM),
            scratch_shapes=[
                pltpu.VMEM((ROUNDS, 2, cy, cz), f32),
                pltpu.VMEM((ROUNDS, 2, cx, cz), f32),
                pltpu.VMEM((ROUNDS, cy, cz), f32),
                pltpu.VMEM((ROUNDS, 2, cy, cz), f32),
                pltpu.VMEM((ROUNDS, 2, cx, cz), f32),
                pltpu.VMEM((ROUNDS, 2, cy, cz), f32),
                pltpu.VMEM((2, cy // 4, cz), f32),
                pltpu.VMEM((2, devices, cy // 4, cz), f32),
                pltpu.VMEM((devices, 8, cz), f32),
                pltpu.VMEM((nx * (cx // 4), rows, wide), f32),
                pltpu.VMEM((nx * (cx // 4), rows, wide), f32),
                pltpu.VMEM((nx * (cx // 4) + 2, rows, wide), f32),
                pltpu.SemaphoreType.DMA((ROUNDS, 6)),
                pltpu.SemaphoreType.DMA((ROUNDS, 6)),
                pltpu.SemaphoreType.DMA((devices,)),
                pltpu.SemaphoreType.DMA((2, devices)),
            ],
            compiler_params=pltpu.CompilerParams(
                collective_id=0, has_side_effects=True, vmem_limit_bytes=60 * 1024 * 1024
            ),
        )(divergence, damping, *tables)

    spec = P(*AXES)
    return jax.shard_map(local, mesh=mesh, in_specs=(spec, spec), out_specs=spec, check_vma=False)
```
